256 devices in a mesh: rows: 128 (over z, y, x), sub: 2 (over core).
Axes of the slice: x: 4, y: 4, z: 8, core: 2. Of those that a mesh axis runs over, the one named last changes fastest.
Arguments:
- matrix: float32 [32768, 384], P(('rows', 'sub')), as said below
- grad_out: float32 [32768, 384], P(('rows', 'sub')), as said below
- grad_factor: float32 [384, 384], replicated, may hold values from -6 to 6
Outputs:
- grad_matrix: float32 [32768, 384], P(('rows', 'sub'))
The draws below stay inside these ranges and needn't reach their ends.
Inputs may be any that keep to these rules, and one draw needn't show every extreme that they name: `matrix`: entries at most of order 1 / sqrt(32768), with a scale that varies by row and by column. `grad_out`: entries of order 0.01.
All inputs are finite; a program needn't handle non-finite values.
Results may differ from the reference program's by a relative error of at most 0.0004.
Values sent between devices are 32-bit elements; how exact they have to be, the bound alone decides.
A program may use at most 64 MiB of HBM per device.

```python
import jax
import jax.numpy as jnp
from jax import lax

N = 384
SECTIONS = 2
R_DEV = 128
ROWS = 32768


def column_mix(key):
    gaussian = jax.random.normal(jax.random.fold_in(key, 15), (N, N), jnp.float32)
    rotation = jnp.linalg.qr(gaussian)[0]
    position = jnp.arange(N, dtype=jnp.float32) / (N - 1)
    column_decay = jnp.power(jnp.float32(10.0), -4.0 * jnp.cbrt(position))
    return column_decay[:, None] * rotation


def shared_rows(key):
    blocks = ROWS // R_DEV
    base_rows = jax.random.normal(jax.random.fold_in(key, 11), (ROWS, N), jnp.float32)
    block_scale = jnp.exp(jax.random.uniform(jax.random.fold_in(key, 13), (blocks, 1), jnp.float32, -0.7, 0.7))
    row_scale = jnp.exp(jax.random.uniform(jax.random.fold_in(key, 14), (ROWS, 1), jnp.float32, -0.5, 0.5))
    scaled = jnp.repeat(block_scale, R_DEV, axis=0) * row_scale
    mixed = jnp.dot(base_rows * scaled, column_mix(key), precision=lax.Precision.HIGHEST, preferred_element_type=jnp.float32)
    return mixed / jnp.sqrt(jnp.float32(ROWS))


def draw_matrix(key, part):
    return shared_rows(key)


def draw_grad_out(key, part):
    noise_rows = jax.random.normal(jax.random.fold_in(key, 21), (ROWS, N), jnp.float32)
    return 0.01 * (noise_rows + 0.03 * jnp.sqrt(jnp.float32(ROWS)) * shared_rows(key))


def normal_values(stream_key, dims, scale, most, held_as=jnp.bfloat16):
    entries = jax.random.normal(stream_key, dims, jnp.float32) * scale
    return jnp.minimum(jnp.maximum(entries, -most), most).astype(held_as)


def setup_inputs(seed: int = 0) -> dict:
    arg_keys = jax.random.split(jax.random.key(seed), 4)
    return {
        "matrix": draw_matrix(jax.random.fold_in(arg_keys[3], 71), 0),
        "grad_out": draw_grad_out(jax.random.fold_in(arg_keys[3], 71), 0),
        "grad_factor": normal_values(arg_keys[2], (N, N), 1.0, 6.0, jnp.float32),
    }


shift_frac = 0.02

def full_dot(left, right):
    return jnp.dot(left.astype(jnp.float32), right.astype(jnp.float32), precision=lax.Precision.HIGHEST, preferred_element_type=jnp.float32)

def inner_gram(left, right):
    return lax.dot_general(left.astype(jnp.float32), right.astype(jnp.float32), (((0,), (0,)), ((), ())), precision=lax.Precision.HIGHEST, preferred_element_type=jnp.float32)

def cholesky_adjoint(lower_fac, lower_inv, lower_grad):
    product = full_dot(lower_fac.T, lower_grad)
    phi_part = jnp.tril(product) - 0.5 * jnp.diag(jnp.diag(product))
    sandwich = full_dot(full_dot(lower_inv.T, phi_part), lower_inv)
    return 0.5 * (sandwich + sandwich.T)

def factor_grads(uppers, grad_factor):
    count = len(uppers)
    result = []
    for section_index in range(count):
        middle = grad_factor
        for later in range(section_index + 1, count):
            middle = full_dot(uppers[later].T, middle)
        for earlier in range(section_index - 1, -1, -1):
            middle = full_dot(middle, uppers[earlier].T)
        result.append(middle)
    return result

def reference(matrix, grad_out, grad_factor):
    width = matrix.shape[1]
    rate = shift_frac / width
    identity = jnp.eye(width, dtype=jnp.float32)
    current = matrix
    saved = []
    for section_index in range(SECTIONS):
        summed = inner_gram(current, current)
        shift_val = rate * jnp.trace(summed)
        lower_fac = jnp.linalg.cholesky(summed + shift_val * identity)
        lower_inv = lax.linalg.triangular_solve(lower_fac, identity, left_side=True, lower=True)
        following = full_dot(current, lower_inv.T)
        saved.append((current, following, lower_fac, lower_inv))
        current = following
    uppers = [item[2].T for item in saved]
    fac_grads = factor_grads(uppers, grad_factor)
    q_grad = grad_out
    for section_index in range(SECTIONS - 1, -1, -1):
        before, after, lower_fac, lower_inv = saved[section_index]
        crossed = inner_gram(after, q_grad)
        total_grad = fac_grads[section_index] - full_dot(crossed, lower_inv)
        gram_grad = cholesky_adjoint(lower_fac, lower_inv, jnp.tril(total_grad.T))
        gram_grad = gram_grad + rate * jnp.trace(gram_grad) * identity
        q_grad = full_dot(q_grad, lower_inv) + 2.0 * full_dot(before, gram_grad)
    return q_grad
```

```python
import jax
import jax.numpy as jnp
from jax import lax
from jax.sharding import Mesh
from jax.sharding import PartitionSpec as P

SECTIONS = 2
ROWS_SUB = ("rows_0", "rows_1", "rows_2", "sub")


shift_frac = 0.02


def in_blocks(shard, dim, count):
    before, after = (shard.shape[:dim], shard.shape[dim + 1 :])
    return jnp.moveaxis(shard.reshape(*before, count, -1, *after), dim, 0)


def sum_at_owner(shard, axis, dim):
    tiles = in_blocks(shard, dim, lax.axis_size(axis))
    arrived = lax.all_to_all(tiles, axis, split_axis=0, concat_axis=0, tiled=True)
    return arrived.sum(axis=0)


def filled_up(lines, count):
    spare = -lines.shape[0] % count
    if not spare:
        return lines
    return jnp.concatenate([lines, jnp.zeros((spare, *lines.shape[1:]), lines.dtype)])


def sent_to_all(shard, axis):
    count = lax.axis_size(axis)
    return lax.all_to_all(
        jnp.broadcast_to(shard[None], (count, *shard.shape)), axis, 0, 0, tiled=True
    )


def laid_out(tiles, dim):
    dims = list(tiles.shape[1:])
    dims[dim] *= tiles.shape[0]
    return jnp.moveaxis(tiles, 0, dim).reshape(dims)


def gathered_by_axis(shard, axes, dim):
    far, near = axes
    leading = sent_to_all(shard, far)
    tiles = jnp.swapaxes(sent_to_all(leading, near), 0, 1)
    return laid_out(tiles.reshape(-1, *shard.shape), dim)


def sum_in_two_steps(shard, axes, dim):
    far, near = axes
    tiles = in_blocks(shard, dim, lax.axis_size(far))
    nearer = sum_at_owner(tiles, near, dim + 1)
    arrived = lax.all_to_all(nearer, far, split_axis=0, concat_axis=0, tiled=True)
    return arrived.sum(axis=0)


def total_of(shard, axes):
    lines = shard.reshape(-1)
    padded = filled_up(lines, lax.axis_size(axes[0]) * lax.axis_size(axes[1]))
    whole = gathered_by_axis(sum_in_two_steps(padded, axes, 0), axes, 0)
    return lax.slice_in_dim(whole, 0, len(lines)).reshape(shard.shape)


def gathered_copies(shard, axis, dim):
    return laid_out(sent_to_all(shard, axis), dim)


def full_dot(left, right):
    return jnp.dot(left, right, precision=lax.Precision.HIGHEST, preferred_element_type=jnp.float32)


def inner_gram(left, right):
    return lax.dot_general(
        left,
        right,
        (((0,), (0,)), ((), ())),
        precision=lax.Precision.HIGHEST,
        preferred_element_type=jnp.float32,
    )


def cholesky_adjoint(lower_fac, lower_inv, lower_grad):
    product = full_dot(lower_fac.T, lower_grad)
    phi_part = jnp.tril(product) - 0.5 * jnp.diag(jnp.diag(product))
    sandwich = full_dot(full_dot(lower_inv.T, phi_part), lower_inv)
    return 0.5 * (sandwich + sandwich.T)


def factor_grads(uppers, grad_factor):
    count = len(uppers)
    result = []
    for section_index in range(count):
        middle = grad_factor
        for later in range(section_index + 1, count):
            middle = full_dot(uppers[later].T, middle)
        for earlier in range(section_index - 1, -1, -1):
            middle = full_dot(middle, uppers[earlier].T)
        result.append(middle)
    return result


def summed_gram(partial_value):
    half_rows = sum_at_owner(partial_value, "sub", 0)
    half_rows = total_of(half_rows, (("rows_0", "rows_1"), "rows_2"))
    return gathered_copies(half_rows, "sub", 0)


def per_device(matrix, grad_out, grad_factor):
    width = matrix.shape[1]
    rate = shift_frac / width
    identity = jnp.eye(width, dtype=jnp.float32)

    def factored(summed):
        shift_val = rate * jnp.trace(summed)
        lower_fac = jnp.linalg.cholesky(summed + shift_val * identity)
        lower_inv = lax.linalg.triangular_solve(lower_fac, identity, left_side=True, lower=True)
        return lower_fac, lower_inv

    def gram_cotangent(total_grad, lower_fac, lower_inv):
        gram_grad = cholesky_adjoint(lower_fac, lower_inv, jnp.tril(total_grad.T))
        return gram_grad + rate * jnp.trace(gram_grad) * identity

    first_fac, first_inv = factored(summed_gram(inner_gram(matrix, matrix)))
    middle = full_dot(matrix, first_inv.T)
    both = summed_gram(inner_gram(middle, jnp.concatenate([middle, grad_out], axis=1)))
    second_gram, crossed = both[:, :width], both[:, width:]
    second_fac, second_inv = factored(second_gram)

    uppers = [first_fac.T, second_fac.T]
    fac_grads = factor_grads(uppers, grad_factor)
    second_total = fac_grads[1] - full_dot(full_dot(second_inv, crossed), second_inv)
    second_weight = gram_cotangent(second_total, second_fac, second_inv)
    first_cross = full_dot(crossed, second_inv) + 2.0 * full_dot(second_gram, second_weight)
    first_total = fac_grads[0] - full_dot(first_cross, first_inv)
    first_weight = gram_cotangent(first_total, first_fac, first_inv)
    middle_grad = full_dot(grad_out, second_inv) + 2.0 * full_dot(middle, second_weight)
    return full_dot(middle_grad, first_inv) + 2.0 * full_dot(matrix, first_weight)


def solution(mesh):
    torus = Mesh(
        mesh.devices.reshape(8, 4, 4, mesh.shape["sub"]), ("rows_0", "rows_1", "rows_2", "sub")
    )
    in_specs = (P(ROWS_SUB, None), P(ROWS_SUB, None), P())
    out_specs = P(ROWS_SUB, None)
    return jax.shard_map(
        per_device, mesh=torus, in_specs=in_specs, out_specs=out_specs, check_vma=False
    )
```

```python
import jax
import jax.numpy as jnp
from jax import lax
from jax.experimental import pallas as pl
from jax.experimental.pallas import tpu as pltpu
from jax.sharding import Mesh
from jax.sharding import PartitionSpec as P

SECTIONS = 2
ROWS_SUB = ("rows_0", "rows_1", "rows_2", "sub")


shift_frac = 0.02


def in_blocks(shard, dim, count):
    before, after = (shard.shape[:dim], shard.shape[dim + 1 :])
    return jnp.moveaxis(shard.reshape(*before, count, -1, *after), dim, 0)


def sum_at_owner(shard, axis, dim):
    tiles = in_blocks(shard, dim, lax.axis_size(axis))
    arrived = lax.all_to_all(tiles, axis, split_axis=0, concat_axis=0, tiled=True)
    return arrived.sum(axis=0)


def filled_up(lines, count):
    spare = -lines.shape[0] % count
    if not spare:
        return lines
    return jnp.concatenate([lines, jnp.zeros((spare, *lines.shape[1:]), lines.dtype)])


def sent_to_all(shard, axis):
    count = lax.axis_size(axis)
    return lax.all_to_all(
        jnp.broadcast_to(shard[None], (count, *shard.shape)), axis, 0, 0, tiled=True
    )


def laid_out(tiles, dim):
    dims = list(tiles.shape[1:])
    dims[dim] *= tiles.shape[0]
    return jnp.moveaxis(tiles, 0, dim).reshape(dims)


def gathered_by_axis(shard, axes, dim):
    far, near = axes
    leading = sent_to_all(shard, far)
    tiles = jnp.swapaxes(sent_to_all(leading, near), 0, 1)
    return laid_out(tiles.reshape(-1, *shard.shape), dim)


def sum_in_two_steps(shard, axes, dim):
    far, near = axes
    tiles = in_blocks(shard, dim, lax.axis_size(far))
    nearer = sum_at_owner(tiles, near, dim + 1)
    arrived = lax.all_to_all(nearer, far, split_axis=0, concat_axis=0, tiled=True)
    return arrived.sum(axis=0)


def total_of(shard, axes):
    lines = shard.reshape(-1)
    padded = filled_up(lines, lax.axis_size(axes[0]) * lax.axis_size(axes[1]))
    whole = gathered_by_axis(sum_in_two_steps(padded, axes, 0), axes, 0)
    return lax.slice_in_dim(whole, 0, len(lines)).reshape(shard.shape)


def gathered_copies(shard, axis, dim):
    return laid_out(sent_to_all(shard, axis), dim)


N = 384
BLOCK = 128
GROUP = 8

def mm(left, right, left_dim=1, right_dim=0):
    return lax.dot_general(left, right, (((left_dim,), (right_dim,)), ((), ())),
        precision=lax.Precision.HIGHEST, preferred_element_type=jnp.float32)

def lanes_of(rows, k):
    return jnp.broadcast_to(rows[:, k:k + 1], (GROUP, BLOCK))

def row_of(rows, k):
    return jnp.broadcast_to(rows[k:k + 1, :], (GROUP, BLOCK))

def factor_block(rows):
    count = BLOCK // GROUP
    row = lax.broadcasted_iota(jnp.int32, (GROUP, BLOCK), 0)
    lane = lax.broadcasted_iota(jnp.int32, (GROUP, BLOCK), 1)
    zero = jnp.zeros((GROUP, BLOCK), jnp.float32)
    rows = list(rows)
    inverse = [jnp.where(lane == row + GROUP * q, 1.0, 0.0) for q in range(count)]
    factor = [zero] * count
    heads = [lanes_of(rows[0], k) for k in range(GROUP)]
    for p in range(count):
        first = GROUP * p
        columns = {q: [lanes_of(rows[q], first + k) for k in range(GROUP)] for q in range(p + 1, count)}
        if p + 1 < count:
            next_heads = [lanes_of(rows[p + 1], first + GROUP + k) for k in range(GROUP)]
        panel, side = rows[p], inverse[p]
        panel_rows, side_rows, roots, scalars = [], [], [], {}
        for j in range(GROUP):
            root = lax.rsqrt(row_of(heads[j], j))
            roots.append(root)
            column = heads[j] * root
            factor[p] = jnp.where((lane == first + j) & (row >= j), column, factor[p])
            below = jnp.where(row > j, column, 0.0)
            for k in range(j + 1, GROUP):
                scalars[k, j] = row_of(heads[k], j) * root
                heads[k] = heads[k] - below * scalars[k, j]
            panel_row = row_of(panel, j) * root
            side_row = row_of(side, j) * root
            panel = panel - below * panel_row
            side = jnp.where(row == j, side_row, side - below * side_row)
            panel_rows.append(panel_row)
            side_rows.append(side_row)
        inverse[p] = side
        for q in range(p + 1, count):
            parts = []
            for k in range(GROUP):
                part = columns[q][k]
                for m in range(k):
                    part = part - parts[m] * scalars[k, m]
                part = part * roots[k]
                parts.append(part)
                factor[q] = jnp.where(lane == first + k, part, factor[q])
            if q == p + 1:
                heads = next_heads
                for k in range(GROUP):
                    for m in range(GROUP):
                        heads[k] = heads[k] - parts[m] * row_of(parts[m], k)
            for k in range(GROUP):
                rows[q] = rows[q] - parts[k] * panel_rows[k]
                inverse[q] = inverse[q] - parts[k] * side_rows[k]
    return factor, inverse

def diagonal_mask():
    return lax.broadcasted_iota(jnp.int32, (N, N), 0) == lax.broadcasted_iota(jnp.int32, (N, N), 1)

def factor_whole(gram, rate, l_ref, v_ref, work, small):
    eye = diagonal_mask()
    shift = rate * jnp.sum(jnp.where(eye, gram, 0.0))
    work[...] = jnp.where(eye, gram + shift, gram)
    l_ref[...] = jnp.zeros((N, N), jnp.float32)
    v_ref[...] = jnp.zeros((N, N), jnp.float32)
    row = lax.broadcasted_iota(jnp.int32, (N, BLOCK), 0)

    def step(b, carry):
        start = pl.multiple_of(b * BLOCK, BLOCK)
        here = pl.ds(start, BLOCK)
        factor, inverse = factor_block(
            [work[pl.ds(start + GROUP * q, GROUP), here] for q in range(BLOCK // GROUP)])
        for q in range(BLOCK // GROUP):
            small[pl.ds(GROUP * q, GROUP), :] = inverse[q]
        mixed = mm(l_ref[here, :], v_ref[...])
        inv = small[...]
        v_ref[here, :] = -mm(inv, mixed)
        v_ref[here, here] = inv
        column = jnp.where(row >= start + BLOCK, mm(work[:, here], inv, 1, 1), 0.0)
        l_ref[:, here] = column
        for q in range(BLOCK // GROUP):
            l_ref[pl.ds(start + GROUP * q, GROUP), here] = factor[q]
        work[...] = work[...] - mm(column, column, 1, 1)
        return carry

    lax.fori_loop(0, N // BLOCK, step, 0)


def inner_gram(left, right):
    return lax.dot_general(
        left,
        right,
        (((0,), (0,)), ((), ())),
        precision=lax.Precision.HIGHEST,
        preferred_element_type=jnp.float32,
    )


def summed_gram(partial_value):
    half_rows = sum_at_owner(partial_value, "sub", 0)
    half_rows = total_of(half_rows, (("rows_0", "rows_1"), "rows_2"))
    return gathered_copies(half_rows, "sub", 0)


def upper_mirrored(square):
    row = lax.broadcasted_iota(jnp.int32, (N, N), 0)
    lane = lax.broadcasted_iota(jnp.int32, (N, N), 1)
    upper = jnp.where(lane > row, square, 0.0)
    return upper + upper.T + jnp.where(lane == row, square, 0.0)


def upper_part(square):
    row = lax.broadcasted_iota(jnp.int32, (N, N), 0)
    lane = lax.broadcasted_iota(jnp.int32, (N, N), 1)
    return jnp.where(lane >= row, square, 0.0)


def gram_cotangent(total_grad, lower_fac, lower_inv, rate):
    mirrored = upper_mirrored(mm(upper_part(total_grad), lower_fac))
    weight = 0.5 * mm(lower_inv.T, mm(mirrored, lower_inv))
    eye = diagonal_mask()
    shift = rate * jnp.sum(jnp.where(eye, weight, 0.0))
    return jnp.where(eye, weight + shift, weight)


def first_kernel(gram, a, g, grad_factor, l1, v1, q1, b2, both, work, small):
    factor_whole(gram[...], shift_frac / N, l1, v1, work, small)
    middle = mm(a[...], v1[...], 1, 1)
    q1[...] = middle
    both[:, :N] = mm(middle, middle, 0, 0)
    both[:, N:] = mm(middle, g[...], 0, 0)
    b2[...] = mm(grad_factor[...], l1[...])


def second_kernel(both, a, g, grad_factor, l1, v1, q1, b2, out, l2, v2, work, small):
    rate = shift_frac / N
    gram, crossed = both[:, :N], both[:, N:]
    factor_whole(gram, rate, l2, v2, work, small)
    fac2, inv2 = l2[...], v2[...]
    weight2 = gram_cotangent(b2[...] - mm(mm(inv2, crossed), inv2), fac2, inv2, rate)
    inv1 = v1[...]
    cross1 = mm(crossed, inv2) + 2.0 * mm(gram, weight2)
    weight1 = gram_cotangent(mm(fac2, grad_factor[...]) - mm(cross1, inv1), l1[...], inv1, rate)
    middle_grad = mm(g[...], inv2) + 2.0 * mm(q1[...], weight2)
    out[...] = mm(middle_grad, inv1) + 2.0 * mm(a[...], weight1)


def local_call(kernel, outs, scratch, name, *operands):
    vmem = pl.BlockSpec(memory_space=pltpu.VMEM)
    return pl.pallas_call(
        kernel,
        out_shape=[jax.ShapeDtypeStruct(shape, jnp.float32) for shape in outs],
        in_specs=[vmem] * len(operands),
        out_specs=[vmem] * len(outs),
        scratch_shapes=[pltpu.VMEM(shape, jnp.float32) for shape in scratch],
        compiler_params=pltpu.CompilerParams(vmem_limit_bytes=48 * 1024 * 1024),
        name=name,
    )(*operands)


def per_device(matrix, grad_out, grad_factor):
    square, rows = (N, N), matrix.shape
    first = summed_gram(inner_gram(matrix, matrix))
    l1, v1, q1, b2, both = local_call(
        first_kernel, [square, square, rows, square, (N, 2 * N)], [square, (BLOCK, BLOCK)],
        "first", first, matrix, grad_out, grad_factor)
    both = summed_gram(both)
    return local_call(
        second_kernel, [rows], [square, square, square, (BLOCK, BLOCK)],
        "second", both, matrix, grad_out, grad_factor, l1, v1, q1, b2)[0]


def solution(mesh):
    torus = Mesh(
        mesh.devices.reshape(8, 4, 4, mesh.shape["sub"]), ("rows_0", "rows_1", "rows_2", "sub")
    )
    in_specs = (P(ROWS_SUB, None), P(ROWS_SUB, None), P())
    out_specs = P(ROWS_SUB, None)
    return jax.shard_map(
        per_device, mesh=torus, in_specs=in_specs, out_specs=out_specs, check_vma=False
    )
```

```python
import jax
import jax.numpy as jnp
from jax import lax
from jax.experimental import pallas as pl
from jax.experimental.pallas import tpu as pltpu
from jax.sharding import Mesh
from jax.sharding import PartitionSpec as P

AXES = ("z", "y", "x", "core")
DEEP, SIDE, PLANE = 8, 4, 16
shift_frac = 0.02
N = 384
BLOCK = 128
GROUP = 8

def mm(left, right, left_dim=1, right_dim=0):
    return lax.dot_general(left, right, (((left_dim,), (right_dim,)), ((), ())),
        precision=lax.Precision.HIGHEST, preferred_element_type=jnp.float32)

def lanes_of(rows, k):
    return jnp.broadcast_to(rows[:, k:k + 1], (GROUP, BLOCK))

def row_of(rows, k):
    return jnp.broadcast_to(rows[k:k + 1, :], (GROUP, BLOCK))

def factor_block(rows):
    count = BLOCK // GROUP
    row = lax.broadcasted_iota(jnp.int32, (GROUP, BLOCK), 0)
    lane = lax.broadcasted_iota(jnp.int32, (GROUP, BLOCK), 1)
    zero = jnp.zeros((GROUP, BLOCK), jnp.float32)
    rows = list(rows)
    inverse = [jnp.where(lane == row + GROUP * q, 1.0, 0.0) for q in range(count)]
    factor = [zero] * count
    heads = [lanes_of(rows[0], k) for k in range(GROUP)]
    for p in range(count):
        first = GROUP * p
        columns = {q: [lanes_of(rows[q], first + k) for k in range(GROUP)] for q in range(p + 1, count)}
        if p + 1 < count:
            next_heads = [lanes_of(rows[p + 1], first + GROUP + k) for k in range(GROUP)]
        panel, side = rows[p], inverse[p]
        panel_rows, side_rows, roots, scalars = [], [], [], {}
        for j in range(GROUP):
            root = lax.rsqrt(row_of(heads[j], j))
            roots.append(root)
            column = heads[j] * root
            factor[p] = jnp.where((lane == first + j) & (row >= j), column, factor[p])
            below = jnp.where(row > j, column, 0.0)
            for k in range(j + 1, GROUP):
                scalars[k, j] = row_of(heads[k], j) * root
                heads[k] = heads[k] - below * scalars[k, j]
            panel_row = row_of(panel, j) * root
            side_row = row_of(side, j) * root
            panel = panel - below * panel_row
            side = jnp.where(row == j, side_row, side - below * side_row)
            panel_rows.append(panel_row)
            side_rows.append(side_row)
        inverse[p] = side
        for q in range(p + 1, count):
            parts = []
            for k in range(GROUP):
                part = columns[q][k]
                for m in range(k):
                    part = part - parts[m] * scalars[k, m]
                part = part * roots[k]
                parts.append(part)
                factor[q] = jnp.where(lane == first + k, part, factor[q])
            if q == p + 1:
                heads = next_heads
                for k in range(GROUP):
                    for m in range(GROUP):
                        heads[k] = heads[k] - parts[m] * row_of(parts[m], k)
            for k in range(GROUP):
                rows[q] = rows[q] - parts[k] * panel_rows[k]
                inverse[q] = inverse[q] - parts[k] * side_rows[k]
    return factor, inverse

def diagonal_mask():
    return lax.broadcasted_iota(jnp.int32, (N, N), 0) == lax.broadcasted_iota(jnp.int32, (N, N), 1)

def factor_whole(gram, rate, l_ref, v_ref, work, small):
    eye = diagonal_mask()
    shift = rate * jnp.sum(jnp.where(eye, gram, 0.0))
    work[...] = jnp.where(eye, gram + shift, gram)
    l_ref[...] = jnp.zeros((N, N), jnp.float32)
    v_ref[...] = jnp.zeros((N, N), jnp.float32)
    row = lax.broadcasted_iota(jnp.int32, (N, BLOCK), 0)

    def step(b, carry):
        start = pl.multiple_of(b * BLOCK, BLOCK)
        here = pl.ds(start, BLOCK)
        factor, inverse = factor_block(
            [work[pl.ds(start + GROUP * q, GROUP), here] for q in range(BLOCK // GROUP)])
        for q in range(BLOCK // GROUP):
            small[pl.ds(GROUP * q, GROUP), :] = inverse[q]
        mixed = mm(l_ref[here, :], v_ref[...])
        inv = small[...]
        v_ref[here, :] = -mm(inv, mixed)
        v_ref[here, here] = inv
        column = jnp.where(row >= start + BLOCK, mm(work[:, here], inv, 1, 1), 0.0)
        l_ref[:, here] = column
        for q in range(BLOCK // GROUP):
            l_ref[pl.ds(start + GROUP * q, GROUP), here] = factor[q]
        work[...] = work[...] - mm(column, column, 1, 1)
        return carry

    lax.fori_loop(0, N // BLOCK, step, 0)


def hops(step):
    return sum(min(part, SIDE - part) for part in (step // SIDE, step % SIDE))


PLANE_STEPS = sorted(range(1, PLANE), key=hops, reverse=True)
DEEP_STEPS = sorted(range(1, DEEP), key=lambda step: min(step, DEEP - step), reverse=True)


def position():
    return tuple(lax.axis_index(name) for name in AXES)


def plane_peer(step, sign):
    z, y, x, core = position()
    return (
        z,
        lax.rem(y + sign * (step // SIDE) + SIDE, SIDE),
        lax.rem(x + sign * (step % SIDE) + SIDE, SIDE),
        core,
    )


def deep_peer(step, sign):
    z, y, x, core = position()
    return (lax.rem(z + sign * step + DEEP, DEEP), y, x, core)


def core_peer():
    z, y, x, core = position()
    return (z, y, x, 1 - core)


def greet():
    barrier = pltpu.get_barrier_semaphore()
    peers = [core_peer()] + [plane_peer(s, 1) for s in PLANE_STEPS] + [deep_peer(s, 1) for s in DEEP_STEPS]
    for peer in peers:
        pl.semaphore_signal(barrier, inc=1, device_id=peer, device_id_type=pl.DeviceIdType.MESH)


def meet():
    pl.semaphore_wait(pltpu.get_barrier_semaphore(), DEEP + PLANE - 1)


def comm_scratch(rows):
    chunk = rows // (2 * PLANE)
    dma = pltpu.SemaphoreType.DMA
    return [
        pltpu.VMEM((rows, BLOCK), jnp.float32),
        pltpu.VMEM((rows // 2, BLOCK), jnp.float32),
        pltpu.VMEM((rows // 2, BLOCK), jnp.float32),
        pltpu.VMEM((PLANE, chunk, BLOCK), jnp.float32),
        pltpu.VMEM((DEEP, chunk, BLOCK), jnp.float32),
        pltpu.VMEM((rows, BLOCK), jnp.float32),
        dma((2, 2)),
        dma((2, PLANE)),
        dma((2, DEEP)),
        dma((2, PLANE)),
        dma((2, 2)),
    ]


def sum_over_devices(packed, half, got, arrived, deep, total, sem_core, sem_plane, sem_deep, sem_out, sem_last, between=None):
    rows = packed.shape[0]
    chunk = rows // (2 * PLANE)
    z, y, x, core = position()
    place = y * SIDE + x
    sent = []

    def send(src, dst, send_sem, recv_sem, peer):
        copy = pltpu.make_async_remote_copy(
            src_ref=src, dst_ref=dst, send_sem=send_sem, recv_sem=recv_sem,
            device_id=peer, device_id_type=pl.DeviceIdType.MESH)
        copy.start()
        sent.append(copy)
        return copy

    def part(ref, index, size):
        return ref.at[pl.ds(pl.multiple_of(index * size, size), size), :]

    send(part(packed, 1 - core, rows // 2), got, sem_core.at[0, 0], sem_core.at[1, 0], core_peer()).wait_recv()
    half[...] = got[...] + packed[pl.ds(pl.multiple_of(core * (rows // 2), rows // 2), rows // 2), :]

    copies = []
    for step in PLANE_STEPS:
        peer = plane_peer(step, 1)
        copies.append(send(part(half, peer[1] * SIDE + peer[2], chunk), arrived.at[step],
                           sem_plane.at[0, step], sem_plane.at[1, step], peer))
    if between is not None:
        between()
    own = half[pl.ds(pl.multiple_of(place * chunk, chunk), chunk), :]
    for copy, step in zip(copies, PLANE_STEPS):
        copy.wait_recv()
    for step in range(1, PLANE):
        own = own + arrived[step]
    deep[z] = own

    copies = []
    for step in DEEP_STEPS:
        copies.append(send(deep.at[z], deep.at[z], sem_deep.at[0, step], sem_deep.at[1, step], deep_peer(step, 1)))
    for step in DEEP_STEPS:
        source = deep_peer(step, -1)[0]
        pltpu.make_async_remote_copy(
            src_ref=deep.at[source], dst_ref=deep.at[source], send_sem=sem_deep.at[0, step],
            recv_sem=sem_deep.at[1, step], device_id=deep_peer(step, -1),
            device_id_type=pl.DeviceIdType.MESH).wait_recv()
    whole = deep[0]
    for index in range(1, DEEP):
        whole = whole + deep[index]
    mine = core * PLANE + place
    total[pl.ds(pl.multiple_of(mine * chunk, chunk), chunk), :] = whole

    for step in PLANE_STEPS:
        spot = part(total, mine, chunk)
        send(spot, spot, sem_out.at[0, step], sem_out.at[1, step], plane_peer(step, 1))
    for step in PLANE_STEPS:
        peer = plane_peer(step, -1)
        spot = part(total, core * PLANE + peer[1] * SIDE + peer[2], chunk)
        pltpu.make_async_remote_copy(
            src_ref=spot, dst_ref=spot, send_sem=sem_out.at[0, step], recv_sem=sem_out.at[1, step],
            device_id=peer, device_id_type=pl.DeviceIdType.MESH).wait_recv()

    spot = part(total, core, rows // 2)
    send(spot, spot, sem_last.at[0, 0], sem_last.at[1, 0], core_peer())
    spot = part(total, 1 - core, rows // 2)
    pltpu.make_async_remote_copy(
        src_ref=spot, dst_ref=spot, send_sem=sem_last.at[0, 0], recv_sem=sem_last.at[1, 0],
        device_id=core_peer(), device_id_type=pl.DeviceIdType.MESH).wait_recv()
    for copy in sent:
        copy.wait_send()


LOWER = [(i, j) for i in range(3) for j in range(i + 1)]
EVERY = [(i, j) for i in range(3) for j in range(3)]


def block_of(ref, i, j):
    return ref.at[pl.ds(i * BLOCK, BLOCK), pl.ds(j * BLOCK, BLOCK)]


def packed_rows(index):
    return pl.ds(index * BLOCK, BLOCK)


def unpack_symmetric(total, out):
    for index, (i, j) in enumerate(LOWER):
        value = total[packed_rows(index), :]
        block_of(out, i, j)[...] = value
        if i != j:
            block_of(out, j, i)[...] = value.T


def first_sum_kernel(a, gram, packed, *scratch):
    greet()
    local = mm(a[...], a[...], 0, 0)
    for index, (i, j) in enumerate(LOWER):
        packed[packed_rows(index), :] = local[i * BLOCK:(i + 1) * BLOCK, j * BLOCK:(j + 1) * BLOCK]
    meet()
    sum_over_devices(packed, *scratch)
    unpack_symmetric(scratch[4], gram)


def second_sum_kernel(a, g, grad_factor, l1, v1, q1, b2, gram, crossed, packed, *scratch):
    greet()
    middle = mm(a[...], v1[...], 1, 1)
    q1[...] = middle
    local = mm(middle, middle, 0, 0)
    for index, (i, j) in enumerate(LOWER):
        packed[packed_rows(index), :] = local[i * BLOCK:(i + 1) * BLOCK, j * BLOCK:(j + 1) * BLOCK]
    local = mm(middle, g[...], 0, 0)
    for index, (i, j) in enumerate(EVERY):
        packed[packed_rows(len(LOWER) + index), :] = local[i * BLOCK:(i + 1) * BLOCK, j * BLOCK:(j + 1) * BLOCK]
    packed[packed_rows(len(LOWER) + len(EVERY)), :] = jnp.zeros((BLOCK, BLOCK), jnp.float32)
    meet()

    def between():
        b2[...] = mm(grad_factor[...], l1[...])

    sum_over_devices(packed, *scratch, between=between)
    total = scratch[4]
    unpack_symmetric(total, gram)
    for index, (i, j) in enumerate(EVERY):
        block_of(crossed, i, j)[...] = total[packed_rows(len(LOWER) + index), :]


def upper_mirrored(square):
    row = lax.broadcasted_iota(jnp.int32, (N, N), 0)
    lane = lax.broadcasted_iota(jnp.int32, (N, N), 1)
    upper = jnp.where(lane > row, square, 0.0)
    return upper + upper.T + jnp.where(lane == row, square, 0.0)


def upper_part(square):
    row = lax.broadcasted_iota(jnp.int32, (N, N), 0)
    lane = lax.broadcasted_iota(jnp.int32, (N, N), 1)
    return jnp.where(lane >= row, square, 0.0)


def gram_cotangent(total_grad, lower_fac, lower_inv, rate):
    mirrored = upper_mirrored(mm(upper_part(total_grad), lower_fac))
    weight = 0.5 * mm(lower_inv.T, mm(mirrored, lower_inv))
    eye = diagonal_mask()
    shift = rate * jnp.sum(jnp.where(eye, weight, 0.0))
    return jnp.where(eye, weight + shift, weight)


def first_kernel(gram, l1, v1, work, small):
    factor_whole(gram[...], shift_frac / N, l1, v1, work, small)


def second_kernel(gram_ref, crossed_ref, a, g, grad_factor, l1, v1, q1, b2, out, l2, v2, work, small):
    rate = shift_frac / N
    gram, crossed = gram_ref[...], crossed_ref[...]
    factor_whole(gram, rate, l2, v2, work, small)
    fac2, inv2 = l2[...], v2[...]
    weight2 = gram_cotangent(b2[...] - mm(mm(inv2, crossed), inv2), fac2, inv2, rate)
    inv1 = v1[...]
    cross1 = mm(crossed, inv2) + 2.0 * mm(gram, weight2)
    weight1 = gram_cotangent(mm(fac2, grad_factor[...]) - mm(cross1, inv1), l1[...], inv1, rate)
    middle_grad = mm(g[...], inv2) + 2.0 * mm(q1[...], weight2)
    out[...] = mm(middle_grad, inv1) + 2.0 * mm(a[...], weight1)


def call(kernel, outs, scratch, name, *operands, **params):
    vmem = pl.BlockSpec(memory_space=pltpu.VMEM)
    return pl.pallas_call(
        kernel,
        out_shape=[jax.ShapeDtypeStruct(shape, jnp.float32) for shape in outs],
        in_specs=[vmem] * len(operands),
        out_specs=[vmem] * len(outs),
        scratch_shapes=scratch,
        compiler_params=pltpu.CompilerParams(vmem_limit_bytes=48 * 1024 * 1024, **params),
        name=name,
    )(*operands)


def per_device(matrix, grad_out, grad_factor):
    square, rows = (N, N), matrix.shape
    work = [pltpu.VMEM(square, jnp.float32), pltpu.VMEM((BLOCK, BLOCK), jnp.float32)]
    (gram1,) = call(first_sum_kernel, [square], comm_scratch(len(LOWER) * BLOCK), "sum1", matrix,
                    collective_id=0, has_side_effects=True)
    l1, v1 = call(first_kernel, [square] * 2, work, "first", gram1)
    q1, b2, gram2, crossed = call(
        second_sum_kernel, [rows, square, square, square], comm_scratch(PLANE * BLOCK), "sum2",
        matrix, grad_out, grad_factor, l1, v1, collective_id=1, has_side_effects=True)
    return call(second_kernel, [rows], [pltpu.VMEM(square, jnp.float32)] * 2 + work, "second",
                gram2, crossed, matrix, grad_out, grad_factor, l1, v1, q1, b2)[0]


def solution(mesh):
    torus = Mesh(mesh.devices.reshape(DEEP, SIDE, SIDE, 2), AXES)
    return jax.shard_map(
        per_device,
        mesh=torus,
        in_specs=(P(AXES, None), P(AXES, None), P()),
        out_specs=P(AXES, None),
        check_vma=False,
    )
```
